32 devices in a mesh: hot: 8 (over z, y), cold: 4 (over x, core).
Axes of the slice: x: 2, y: 2, z: 4, core: 2. Of those that a mesh axis runs over, the one named last changes fastest.
Arguments:
- tokens: bfloat16 [64, 8192], replicated, may hold values from -6 to 6
- norm_gain: float32 [8192], replicated, may hold values from 0.1 to 1.9
- hot_gate: bfloat16 [512, 8192], P(('hot', 'cold')), may hold values from -0.0625 to 0.0625
- hot_up: bfloat16 [512, 8192], P(('hot', 'cold')), may hold values from -0.0625 to 0.0625
- hot_down: bfloat16 [512, 8192], P(('hot', 'cold')), may hold values from -0.09375 to 0.09375
- hot_index: int32 [512], replicated, may hold values from 0 to 14335, as said below
- cold_gate: bfloat16 [8192, 14336], P('hot', 'cold'), may hold values from -0.0625 to 0.0625
- cold_up: bfloat16 [8192, 14336], P('hot', 'cold'), may hold values from -0.0625 to 0.0625
- cold_down: bfloat16 [14336, 8192], P('cold', 'hot'), may hold values from -0.0625 to 0.0625
- block_mask: int32 [64, 112], P(None, 'cold'), may hold values from 0 to 1, as said below
Outputs:
- ffn_out: bfloat16 [64, 8192], P(None, ('hot', 'cold'))
The draws below stay inside these ranges and needn't reach their ends.
Inputs may be any that keep to these rules, and one draw needn't show every extreme that they name: `hot_index`: distinct hidden units. `block_mask`: in each run of 28 blocks held by one index of cold, at most 14 blocks are active for any sequence, and some index reaches exactly 14.
All inputs are finite; a program needn't handle non-finite values.
Results may differ from the reference program's by a relative error of at most 0.0065.
Values may be sent and summed in bfloat16 or wider, within the bound.
No kernel may reach another device: no remote copies, remote signals or barrier semaphores. Data moves between devices by JAX's collectives and lax.ppermute only.
A program may use at most 64 MiB of HBM per device.

```python
import jax
import jax.numpy as jnp
from jax import lax

D = 8192
UNITS = 14336
BLOCK = 128
SEQ = 64
HOT = 512
BLOCKS = 112
BLK_DEV = 28
CAP = 14


def draw_hot_index(key, part):
    return jax.random.permutation(jax.random.fold_in(key, 11), UNITS)[:HOT].astype(jnp.int32)


def draw_block_mask(key, part):
    groups = BLOCKS // BLK_DEV
    key_busy, key_count, key_rank, key_bits = jax.random.split(jax.random.fold_in(key, 23), 4)
    busy = jax.random.randint(key_busy, (), 0, groups)
    counts = jax.random.randint(key_count, (groups,), CAP // 8, CAP // 3 + 1)
    counts = jnp.where(jnp.arange(groups) == busy, CAP, counts)
    scores = jax.random.randint(key_rank, (groups, BLK_DEV), 0, 1048576) * BLK_DEV + jnp.arange(BLK_DEV)[None, :]
    ranks = jnp.argsort(jnp.argsort(scores, axis=1), axis=1)
    active = (ranks < counts[:, None]).astype(jnp.int32).reshape(BLOCKS)
    bits = jax.random.randint(key_bits, (SEQ, BLOCKS), 0, 2)
    forced = (jnp.arange(SEQ)[:, None] == (jnp.arange(BLOCKS) % SEQ)[None, :]).astype(jnp.int32)
    return (active[None, :] * jnp.maximum(bits, forced)).astype(jnp.int32)


def strengthened(array, rng, source, target, blocks, factor):
    owner, partner = [(jnp.arange(array.shape[dim]) // (array.shape[dim] // blocks)).reshape([-1 if axis == dim else 1 for axis in range(array.ndim)]) for dim in (source, target)]
    chosen = jax.random.permutation(rng, blocks)[partner]
    strong = (owner == chosen) | (owner == (partner + blocks // 2) % blocks)
    return jnp.where(strong, factor * array, array)


def level_of(stream_key, shape, pieces, least, top_value):
    gain = 1.0
    for position, blocks in pieces:
        draws = jax.random.uniform(jax.random.fold_in(jax.random.fold_in(stream_key, 6), position), (blocks,), jnp.float32, least / len(pieces), top_value / len(pieces))
        gain = gain * jnp.repeat(jnp.exp(draws), shape[position] // blocks).reshape((-1,) + (1,) * (len(shape) - 1 - position))
    return gain


def centred(own_key, shape, deviation, bound, shards=(), dtype=jnp.bfloat16):
    values = jax.random.normal(own_key, shape, jnp.float32) * deviation
    if len(shards) > 0:
        values = level_of(own_key, shape, shards, -0.22, 0.18) * values
    return jnp.clip(values, min=-bound, max=bound).astype(dtype)


def heavy_noise(rng, extent, scale, reach, shards, heavy, kind=jnp.bfloat16):
    entries = scale * jax.random.normal(rng, extent, jnp.float32)
    if shards:
        entries = entries * level_of(rng, extent, shards, -0.22, 0.18)
    return jnp.clip(strengthened(entries, jax.random.fold_in(rng, 3), *heavy), -reach, reach).astype(kind)


def setup_inputs(seed: int = 0) -> dict:
    seeds = jax.random.split(jax.random.key(seed), 11)
    tokens = centred(seeds[0], (SEQ, D), 1.0, 6.0)
    norm_gain = jnp.clip(1.0 + 0.18 * jax.random.normal(seeds[1], (D,), jnp.float32), 0.1, 1.9)
    hot_gate = centred(seeds[2], (HOT, D), D ** -0.5, 0.0625, ((0, 32),))
    hot_up = centred(seeds[3], (HOT, D), D ** -0.5, 0.0625, ((0, 32),))
    hot_down = heavy_noise(seeds[4], (HOT, D), UNITS ** -0.5, 0.09375, ((0, 32),), (0, 1, 32, 2.75))
    hot_index = draw_hot_index(jax.random.fold_in(seeds[10], 71), 0)
    cold_gate = centred(seeds[6], (D, UNITS), D ** -0.5, 0.0625, ((0, 8), (1, 4)))
    cold_up = centred(seeds[7], (D, UNITS), D ** -0.5, 0.0625, ((0, 8), (1, 4)))
    cold_down = heavy_noise(seeds[8], (UNITS, D), UNITS ** -0.5, 0.0625, ((0, 4), (1, 8)), (0, 1, 8, 2.0))
    block_mask = draw_block_mask(jax.random.fold_in(seeds[10], 71), 0)
    return {"tokens": tokens, "norm_gain": norm_gain, "hot_gate": hot_gate, "hot_up": hot_up, "hot_down": hot_down, "hot_index": hot_index, "cold_gate": cold_gate, "cold_up": cold_up, "cold_down": cold_down, "block_mask": block_mask}


def reference(tokens, norm_gain, hot_gate, hot_up, hot_down, hot_index, cold_gate, cold_up, cold_down, block_mask):
    values = tokens.astype(jnp.float32)
    scale = lax.rsqrt(lax.optimization_barrier(jnp.mean(values * values, axis=1, keepdims=True)) + 1e-05)
    normed = (values * scale * norm_gain.astype(jnp.float32)[None, :]).astype(jnp.bfloat16)
    dims = (((1,), (1,)), ((), ()))
    gate_hot = lax.dot_general(normed, hot_gate, dims, preferred_element_type=jnp.float32)
    up_hot = lax.dot_general(normed, hot_up, dims, preferred_element_type=jnp.float32)
    hidden_hot = (jax.nn.silu(gate_hot) * up_hot).astype(jnp.bfloat16)
    out_hot = jnp.dot(hidden_hot, hot_down, preferred_element_type=jnp.float32)
    is_hot = jnp.zeros((UNITS,), jnp.float32).at[hot_index.astype(jnp.int32)].set(1.0)
    live = jnp.repeat(block_mask, BLOCK, axis=1).astype(jnp.float32) * (1.0 - is_hot)[None, :]
    gate_cold = jnp.dot(normed, cold_gate, preferred_element_type=jnp.float32)
    up_cold = jnp.dot(normed, cold_up, preferred_element_type=jnp.float32)
    hidden_cold = (jax.nn.silu(gate_cold) * up_cold * live).astype(jnp.bfloat16)
    out_cold = jnp.dot(hidden_cold, cold_down, preferred_element_type=jnp.float32)
    return (out_hot + out_cold).astype(jnp.bfloat16)
```

```python
import functools

import jax
import jax.numpy as jnp
from jax import lax
from jax.experimental import pallas as pl
from jax.experimental.pallas import tpu as pltpu
from jax.sharding import PartitionSpec as P

F32 = jnp.float32
BF16 = jnp.bfloat16
ANY = pl.BlockSpec(memory_space=pl.ANY)
VMEM = pl.BlockSpec(memory_space=pltpu.VMEM)
SMEM = pl.BlockSpec(memory_space=pltpu.SMEM)
NT = (((1,), (1,)), ((), ()))


def silu(v):
    return v / (1.0 + jnp.exp(-v))


def partial_kernel(
    tokens, gain, hot_gate, hot_up, hot_index, cold_gate, cold_up, mask,
    out, live, picks,
    tok_v, gain_v, hot_v, hidx_v, mask_v, normed_v, unit_v, w_v, in_sem, w_sem,
    *, slots, block, n_hot,
):
    seqs, width = tok_v.shape
    feats = cold_gate.shape[0]
    blocks = mask.shape[1]
    rows = hot_gate.shape[0]
    h = lax.axis_index("hot")
    c = lax.axis_index("cold")
    loads = [
        pltpu.make_async_copy(mask, mask_v, in_sem.at[0]),
        pltpu.make_async_copy(tokens, tok_v, in_sem.at[1]),
        pltpu.make_async_copy(gain, gain_v, in_sem.at[2]),
        pltpu.make_async_copy(hot_index, hidx_v, in_sem.at[3]),
        pltpu.make_async_copy(hot_gate, hot_v.at[pl.ds(0, rows)], in_sem.at[4]),
        pltpu.make_async_copy(hot_up, hot_v.at[pl.ds(rows, rows)], in_sem.at[5]),
    ]
    for load in loads:
        load.start()
    loads[0].wait()
    alive = jnp.max(mask_v[...].astype(F32), axis=0, keepdims=True)
    tri = (
        lax.broadcasted_iota(jnp.int32, (blocks, blocks), 0)
        <= lax.broadcasted_iota(jnp.int32, (blocks, blocks), 1)
    ).astype(F32)
    rank = jnp.dot(jnp.broadcast_to(alive, (8, blocks)), tri, preferred_element_type=F32)[:1]
    rank = jnp.where(alive > 0.0, rank, 0.0)
    lane = lax.broadcasted_iota(jnp.int32, (1, blocks), 1)
    lane_f = lane.astype(F32)
    count = jnp.sum(alive).astype(jnp.int32)
    picks[slots] = count
    index = []
    for j in range(slots):
        index.append(jnp.sum(jnp.where(rank == float(j + 1), lane_f, 0.0)).astype(jnp.int32))

    def copies(j):
        cols = pl.ds(pl.multiple_of(index[j] * block, block), block)
        return (
            pltpu.make_async_copy(
                cold_gate.at[:, cols], w_v.at[j, :, pl.ds(0, block)], w_sem.at[0, j]
            ),
            pltpu.make_async_copy(
                cold_up.at[:, cols], w_v.at[j, :, pl.ds(block, block)], w_sem.at[1, j]
            ),
        )

    for j in range(slots):
        picks[j] = index[j]

        @pl.when(j < count)
        def _():
            for copy in copies(j):
                copy.start()

    loads[1].wait()
    loads[2].wait()
    values = tok_v[...].astype(F32)
    scale = lax.rsqrt(jnp.mean(values * values, axis=1, keepdims=True) + 1e-05)
    normed_v[...] = (values * scale * gain_v[...]).astype(BF16)

    loads[3].wait()
    hidx = hidx_v[...] - c * (blocks * block)
    owner = lax.shift_right_arithmetic(hidx, jnp.int32(block.bit_length() - 1))
    inner = jnp.bitwise_and(hidx, jnp.int32(block - 1))
    n = hidx.shape[1]
    by_block = (lax.broadcasted_iota(jnp.int32, (blocks, n), 0) == owner).astype(F32)
    by_unit = (lax.broadcasted_iota(jnp.int32, (block, n), 0) == inner).astype(F32)
    unit_v[...] = 1.0 - lax.dot_general(by_block, by_unit, NT, preferred_element_type=F32)
    chunk = live.shape[0]
    seq_mask = mask_v[pl.ds(h * chunk, chunk), :].astype(F32)
    for j in range(slots):
        seq_live = jnp.sum(
            jnp.where(lane == index[j], seq_mask, 0.0), axis=1, keepdims=True
        ) * jnp.where(j < count, 1.0, 0.0)
        live[:, pl.ds(j * block, block)] = seq_live * unit_v[pl.ds(index[j], 1), :]

    loads[4].wait()
    loads[5].wait()
    both = lax.dot_general(normed_v[...], hot_v[...], NT, preferred_element_type=F32)
    hidden_hot = (silu(both[:, :rows]) * both[:, rows:]).astype(BF16)
    spread = (
        lax.broadcasted_iota(jnp.int32, (rows, rows * n_hot), 1)
        == lax.broadcasted_iota(jnp.int32, (rows, rows * n_hot), 0) + h * rows
    ).astype(BF16)
    out[:, pl.ds(2 * slots * block, rows * n_hot)] = jnp.dot(
        hidden_hot, spread, preferred_element_type=F32
    ).astype(BF16)

    part = normed_v[:, pl.ds(pl.multiple_of(h * feats, feats), feats)]
    for j in range(slots):
        cols = pl.ds(2 * j * block, 2 * block)

        @pl.when(j < count)
        def _():
            for copy in copies(j):
                copy.wait()
            out[:, cols] = jnp.dot(part, w_v[j], preferred_element_type=F32).astype(BF16)

        @pl.when(j >= count)
        def _():
            out[:, cols] = jnp.zeros((seqs, 2 * block), BF16)


def hidden_kernel(parts, live, out, *, slots, block, n_hot):
    chunk = live.shape[0]
    total = parts[pl.ds(0, chunk), :].astype(F32)
    for src in range(1, n_hot):
        total = total + parts[pl.ds(src * chunk, chunk), :].astype(F32)
    pieces = []
    for j in range(slots):
        gate = total[:, 2 * j * block : (2 * j + 1) * block]
        up = total[:, (2 * j + 1) * block : (2 * j + 2) * block]
        pieces.append((silu(gate) * up * live[:, pl.ds(j * block, block)]).astype(BF16))
    pieces.append(total[:, 2 * slots * block :].astype(BF16))
    hidden = jnp.concatenate(pieces, axis=1)
    for dst in range(n_hot):
        out[pl.ds(dst * chunk, chunk), :] = hidden


def down_kernel(picks, hidden, hot_rows, cold_down, out, w_v, sem, hot_sem, *, slots, block):
    count = picks[slots]
    base = slots * block

    def copy(j):
        rows = pl.ds(pl.multiple_of(picks[j] * block, block), block)
        return pltpu.make_async_copy(
            cold_down.at[rows], w_v.at[pl.ds(j * block, block)], sem.at[j]
        )

    hot_copy = pltpu.make_async_copy(hot_rows, w_v.at[pl.ds(base, hot_rows.shape[0])], hot_sem.at[0])
    for j in range(slots):

        @pl.when(j < count)
        def _():
            copy(j).start()

        @pl.when(j >= count)
        def _():
            w_v[pl.ds(j * block, block), :] = jnp.zeros((block, w_v.shape[1]), BF16)

    hot_copy.start()
    for j in range(slots):

        @pl.when(j < count)
        def _():
            copy(j).wait()

    hot_copy.wait()
    total = jnp.dot(hidden[...], w_v[...], preferred_element_type=F32)
    n_cold, _, cols = out.shape
    for k in range(n_cold):
        out[k] = total[:, k * cols : (k + 1) * cols].astype(out.dtype)


def on_device(
    tokens, norm_gain, hot_gate, hot_up, hot_down, hot_index,
    cold_gate, cold_up, cold_down, block_mask, *, n_hot, n_cold,
):
    seqs, width = tokens.shape
    feats, units = cold_gate.shape
    blocks = block_mask.shape[1]
    block = units // blocks
    slots = blocks // 2
    rows = hot_gate.shape[0]
    hots = hot_index.shape[0]
    chunk = seqs // n_hot
    hot_lanes = rows * n_hot
    cols = cold_down.shape[1]

    down_rows = lax.all_to_all(hot_down, "hot", split_axis=1, concat_axis=0, tiled=True)

    parts, live, picks = pl.pallas_call(
        functools.partial(partial_kernel, slots=slots, block=block, n_hot=n_hot),
        name="partial",
        in_specs=[ANY] * 8,
        out_specs=[VMEM, VMEM, SMEM],
        out_shape=[
            jax.ShapeDtypeStruct((seqs, 2 * slots * block + hot_lanes), BF16),
            jax.ShapeDtypeStruct((chunk, slots * block), F32),
            jax.ShapeDtypeStruct((slots + 1,), jnp.int32),
        ],
        scratch_shapes=[
            pltpu.VMEM((seqs, width), BF16),
            pltpu.VMEM((1, width), F32),
            pltpu.VMEM((2 * rows, width), BF16),
            pltpu.VMEM((1, hots), jnp.int32),
            pltpu.VMEM((seqs, blocks), jnp.int32),
            pltpu.VMEM((seqs, width), BF16),
            pltpu.VMEM((blocks, block), F32),
            pltpu.VMEM((slots, feats, 2 * block), BF16),
            pltpu.SemaphoreType.DMA((6,)),
            pltpu.SemaphoreType.DMA((2, slots)),
        ],
    )(
        tokens, norm_gain[None, :], hot_gate, hot_up, hot_index[None, :],
        cold_gate, cold_up, block_mask,
    )
    parts = lax.all_to_all(parts, "hot", split_axis=0, concat_axis=0, tiled=True)
    hidden = pl.pallas_call(
        functools.partial(hidden_kernel, slots=slots, block=block, n_hot=n_hot),
        name="hidden",
        in_specs=[VMEM, VMEM],
        out_specs=VMEM,
        out_shape=jax.ShapeDtypeStruct((seqs, slots * block + hot_lanes), BF16),
    )(parts, live)
    hidden = lax.all_to_all(hidden, "hot", split_axis=0, concat_axis=0, tiled=True)
    out = pl.pallas_call(
        functools.partial(down_kernel, slots=slots, block=block),
        name="down",
        in_specs=[SMEM, VMEM, ANY, ANY],
        out_specs=VMEM,
        out_shape=jax.ShapeDtypeStruct((n_cold, seqs, cols // n_cold), BF16),
        scratch_shapes=[
            pltpu.VMEM((slots * block + hot_lanes, cols), BF16),
            pltpu.SemaphoreType.DMA((slots,)),
            pltpu.SemaphoreType.DMA((1,)),
        ],
    )(picks, hidden, down_rows, cold_down)
    out = lax.all_to_all(out, "cold", split_axis=0, concat_axis=0, tiled=True)
    return jnp.sum(out.astype(F32), axis=0).astype(BF16)


def solution(mesh):
    in_specs = (
        P(),
        P(),
        P(("hot", "cold"), None),
        P(("hot", "cold"), None),
        P(("hot", "cold"), None),
        P(),
        P("hot", "cold"),
        P("hot", "cold"),
        P("cold", "hot"),
        P(None, "cold"),
    )
    body = functools.partial(on_device, n_hot=mesh.shape["hot"], n_cold=mesh.shape["cold"])
    return jax.shard_map(
        body, mesh=mesh, in_specs=in_specs, out_specs=P(None, ("hot", "cold")), check_vma=False
    )
```

```python
import functools

import jax
import jax.numpy as jnp
from jax import lax
from jax.experimental import pallas as pl
from jax.experimental.pallas import tpu as pltpu
from jax.sharding import PartitionSpec as P


F32 = jnp.float32
BF16 = jnp.bfloat16
ANY = pl.BlockSpec(memory_space=pl.ANY)
VMEM = pl.BlockSpec(memory_space=pltpu.VMEM)
SMEM = pl.BlockSpec(memory_space=pltpu.SMEM)
NT = (((1,), (1,)), ((), ()))


def limit(mib):
    return pltpu.CompilerParams(vmem_limit_bytes=mib << 20)


def silu(v):
    return v / (1.0 + jnp.exp(-v))


def partial_kernel(
    tokens_hbm, gain_hbm, hot_gate_hbm, hot_up_hbm, hot_index_hbm, mask_hbm, cold_gate, cold_up,
    out, live, picks,
    tokens, gain, hot_gate, hot_up, hot_index, mask, normed_v, unit_v, w_v, in_sem, w_sem,
    *, slots, block, n_hot,
):
    loads = [
        pltpu.make_async_copy(source, target, in_sem.at[i])
        for i, (source, target) in enumerate((
            (mask_hbm, mask), (tokens_hbm, tokens), (gain_hbm, gain),
            (hot_index_hbm, hot_index), (hot_gate_hbm, hot_gate), (hot_up_hbm, hot_up),
        ))
    ]
    for load in loads:
        load.start()
    loads[0].wait()
    seqs = tokens.shape[0]
    feats = cold_gate.shape[0]
    blocks = mask.shape[0]
    rows = hot_gate.shape[0]
    h = lax.axis_index("hot")
    c = lax.axis_index("cold")
    mask_f = mask[...].astype(F32)
    alive = jnp.max(mask_f, axis=1, keepdims=True)
    tri = (
        lax.broadcasted_iota(jnp.int32, (blocks, blocks), 1)
        <= lax.broadcasted_iota(jnp.int32, (blocks, blocks), 0)
    ).astype(F32)
    rank = jnp.dot(tri, jnp.broadcast_to(alive, (blocks, block)), preferred_element_type=F32)
    rank = jnp.where(alive > 0.0, rank[:, :1], 0.0)
    number = lax.broadcasted_iota(jnp.int32, (blocks, 1), 0).astype(F32)
    count = jnp.sum(alive).astype(jnp.int32)
    picks[slots] = count
    index = []
    for j in range(slots):
        index.append(jnp.sum(jnp.where(rank == float(j + 1), number, 0.0)).astype(jnp.int32))

    def copies(j):
        cols = pl.ds(pl.multiple_of(index[j] * block, block), block)
        return (
            pltpu.make_async_copy(
                cold_gate.at[:, cols], w_v.at[j, :, pl.ds(0, block)], w_sem.at[0, j]
            ),
            pltpu.make_async_copy(
                cold_up.at[:, cols], w_v.at[j, :, pl.ds(block, block)], w_sem.at[1, j]
            ),
        )

    for j in range(slots):
        picks[j] = index[j]

        @pl.when(j < count)
        def _():
            for copy in copies(j):
                copy.start()

    loads[1].wait()
    loads[2].wait()
    values = tokens[...].astype(F32)
    scale = lax.rsqrt(jnp.mean(values * values, axis=1, keepdims=True) + 1e-05)
    normed_v[...] = (values * scale * gain[...]).astype(BF16)

    loads[3].wait()
    hidx = hot_index[...] - c * (blocks * block)
    owner = lax.shift_right_arithmetic(hidx, jnp.int32(block.bit_length() - 1))
    inner = jnp.bitwise_and(hidx, jnp.int32(block - 1))
    n = hidx.shape[1]
    by_block = (lax.broadcasted_iota(jnp.int32, (blocks, n), 0) == owner).astype(F32)
    by_unit = (lax.broadcasted_iota(jnp.int32, (block, n), 0) == inner).astype(F32)
    unit_v[...] = 1.0 - lax.dot_general(by_block, by_unit, NT, preferred_element_type=F32)
    chunk = live.shape[0]
    mine = (
        lax.broadcasted_iota(jnp.int32, (chunk, seqs), 1)
        == lax.broadcasted_iota(jnp.int32, (chunk, seqs), 0) + h * chunk
    ).astype(F32)
    seq_mask = lax.dot_general(mine, mask_f, NT, preferred_element_type=F32)
    lane = lax.broadcasted_iota(jnp.int32, (1, blocks), 1)
    for j in range(slots):
        seq_live = jnp.sum(
            jnp.where(lane == index[j], seq_mask, 0.0), axis=1, keepdims=True
        ) * jnp.where(j < count, 1.0, 0.0)
        live[:, pl.ds(j * block, block)] = seq_live * unit_v[pl.ds(index[j], 1), :]

    loads[4].wait()
    loads[5].wait()
    gate_hot = lax.dot_general(normed_v[...], hot_gate[...], NT, preferred_element_type=F32)
    up_hot = lax.dot_general(normed_v[...], hot_up[...], NT, preferred_element_type=F32)
    hidden_hot = (silu(gate_hot) * up_hot).astype(BF16)
    spread = (
        lax.broadcasted_iota(jnp.int32, (rows, rows * n_hot), 1)
        == lax.broadcasted_iota(jnp.int32, (rows, rows * n_hot), 0) + h * rows
    ).astype(BF16)
    out[:, pl.ds(2 * slots * block, rows * n_hot)] = jnp.dot(
        hidden_hot, spread, preferred_element_type=F32
    ).astype(BF16)

    part = normed_v[:, pl.ds(pl.multiple_of(h * feats, feats), feats)]
    for j in range(slots):
        cols = pl.ds(2 * j * block, 2 * block)

        @pl.when(j < count)
        def _():
            for copy in copies(j):
                copy.wait()
            out[:, cols] = jnp.dot(part, w_v[j], preferred_element_type=F32).astype(BF16)

        @pl.when(j >= count)
        def _():
            out[:, cols] = jnp.zeros((seqs, 2 * block), BF16)


def hidden_kernel(parts, live, out, *, slots, block, n_hot):
    chunk = live.shape[0]
    total = parts[pl.ds(0, chunk), :].astype(F32)
    for src in range(1, n_hot):
        total = total + parts[pl.ds(src * chunk, chunk), :].astype(F32)
    pieces = []
    for j in range(slots):
        gate = total[:, 2 * j * block : (2 * j + 1) * block]
        up = total[:, (2 * j + 1) * block : (2 * j + 2) * block]
        pieces.append((silu(gate) * up * live[:, pl.ds(j * block, block)]).astype(BF16))
    pieces.append(total[:, 2 * slots * block :].astype(BF16))
    hidden = jnp.concatenate(pieces, axis=1)
    for dst in range(n_hot):
        out[pl.ds(dst * chunk, chunk), :] = hidden


def down_kernel(picks, hidden, hot_rows, cold_down, own, *rest, slots, block):
    sends, (total, w, sem) = rest[:-3], rest[-3:]
    count = picks[slots]
    group = 2 if slots % 2 == 0 else 1

    def copy(j):
        rows = pl.ds(pl.multiple_of(picks[j] * block, block), block)
        return pltpu.make_async_copy(cold_down.at[rows], w.at[pl.ds(j * block, block)], sem.at[j])

    for j in range(slots):

        @pl.when(j < count)
        def _():
            copy(j).start()

        @pl.when(j >= count)
        def _():
            w[pl.ds(j * block, block), :] = jnp.zeros((block, w.shape[1]), BF16)

    base = slots * block
    total[...] = jnp.dot(
        hidden[:, pl.ds(base, hot_rows.shape[0])], hot_rows[...], preferred_element_type=F32
    )
    for first in range(0, slots, group):

        @pl.when(first < count)
        def _():
            for j in range(first, first + group):

                @pl.when(j < count)
                def _():
                    copy(j).wait()

            rows = pl.ds(first * block, group * block)
            total[...] += jnp.dot(hidden[:, rows], w[rows, :], preferred_element_type=F32)

    c = lax.axis_index("cold")
    cols = own.shape[1]

    def piece(k):
        if cols % 128 == 0:
            return total[:, pl.ds(pl.multiple_of(k * cols, cols), cols)]
        value = jnp.zeros((total.shape[0], cols), F32)
        for i in range(total.shape[1] // cols):
            value = jnp.where(k == i, total[:, i * cols : (i + 1) * cols], value)
        return value

    own[...] = piece(c)
    for k, send in enumerate(sends):
        send[...] = piece(jnp.bitwise_xor(c, k + 1)).astype(send.dtype)


def in_vmem(value):
    return pltpu.with_memory_space_constraint(value, pltpu.VMEM)


def in_hbm(value):
    return pltpu.with_memory_space_constraint(value, pltpu.HBM)


def on_device(
    tokens, norm_gain, hot_gate, hot_up, hot_down, hot_index,
    cold_gate, cold_up, cold_down, block_mask, *, n_hot, n_cold,
):
    seqs, width = tokens.shape
    feats, units = cold_gate.shape
    blocks = block_mask.shape[1]
    block = units // blocks
    slots = blocks // 2
    rows = hot_gate.shape[0]
    chunk = seqs // n_hot
    hot_lanes = rows * n_hot
    cols = cold_down.shape[1]

    hot_rows = lax.all_to_all(hot_down, "hot", split_axis=1, concat_axis=0, tiled=True)

    parts, live, picks = pl.pallas_call(
        functools.partial(partial_kernel, slots=slots, block=block, n_hot=n_hot),
        name="partial",
        compiler_params=limit(20),
        in_specs=[ANY] * 8,
        out_specs=[VMEM, VMEM, SMEM],
        out_shape=[
            pltpu.VMEM((seqs, 2 * slots * block + hot_lanes), BF16),
            pltpu.VMEM((chunk, slots * block), F32),
            jax.ShapeDtypeStruct((slots + 1,), jnp.int32),
        ],
        scratch_shapes=[
            pltpu.VMEM((seqs, width), BF16),
            pltpu.VMEM((1, width), F32),
            pltpu.VMEM((rows, width), BF16),
            pltpu.VMEM((rows, width), BF16),
            pltpu.VMEM((1, hot_index.shape[0]), jnp.int32),
            pltpu.VMEM((blocks, seqs), jnp.int32),
            pltpu.VMEM((seqs, width), BF16),
            pltpu.VMEM((blocks, block), F32),
            pltpu.VMEM((slots, feats, 2 * block), BF16),
            pltpu.SemaphoreType.DMA((6,)),
            pltpu.SemaphoreType.DMA((2, slots)),
        ],
    )(*(in_hbm(value) for value in (
        tokens, norm_gain[None, :], hot_gate, hot_up, hot_index[None, :],
        block_mask.T, cold_gate, cold_up,
    )))
    parts, hot_rows = lax.optimization_barrier((parts, hot_rows))
    parts = lax.all_to_all(parts, "hot", split_axis=0, concat_axis=0, tiled=True)
    hidden = pl.pallas_call(
        functools.partial(hidden_kernel, slots=slots, block=block, n_hot=n_hot),
        name="hidden",
        compiler_params=limit(8),
        in_specs=[VMEM, VMEM],
        out_specs=VMEM,
        out_shape=pltpu.VMEM((seqs, slots * block + hot_lanes), BF16),
    )(in_vmem(parts), in_vmem(live))
    hidden = lax.all_to_all(hidden, "hot", split_axis=0, concat_axis=0, tiled=True)
    piece = (seqs, cols // n_cold)
    own, *sends = pl.pallas_call(
        functools.partial(down_kernel, slots=slots, block=block),
        name="down",
        compiler_params=limit(8),
        in_specs=[SMEM, VMEM, VMEM, ANY],
        out_specs=[VMEM] * n_cold,
        out_shape=[pltpu.VMEM(piece, F32)] + [pltpu.VMEM(piece, BF16)] * (n_cold - 1),
        scratch_shapes=[
            pltpu.VMEM((seqs, cols), F32),
            pltpu.VMEM((slots * block, cols), BF16),
            pltpu.SemaphoreType.DMA((slots,)),
        ],
    )(picks, in_vmem(hidden), in_vmem(hot_rows), in_hbm(cold_down))
    for k, send in enumerate(sends):
        got = lax.ppermute(send, "cold", [(i, i ^ (k + 1)) for i in range(n_cold)])
        own = own + got.astype(F32)
    return own.astype(BF16)


def solution(mesh):
    in_specs = (
        P(),
        P(),
        P(("hot", "cold"), None),
        P(("hot", "cold"), None),
        P(("hot", "cold"), None),
        P(),
        P("hot", "cold"),
        P("hot", "cold"),
        P("cold", "hot"),
        P(None, "cold"),
    )

    def body(*args):
        return on_device(*args, n_hot=mesh.shape["hot"], n_cold=mesh.shape["cold"])

    return jax.shard_map(
        body, mesh=mesh, in_specs=in_specs, out_specs=P(None, ("hot", "cold")), check_vma=False
    )
```

```python
import functools

import jax
import jax.numpy as jnp
from jax import lax
from jax.experimental import pallas as pl
from jax.experimental.pallas import tpu as pltpu
from jax.sharding import PartitionSpec as P

F32 = jnp.float32
BF16 = jnp.bfloat16
ANY = pl.BlockSpec(memory_space=pl.ANY)
VMEM = pl.BlockSpec(memory_space=pltpu.VMEM)
SMEM = pl.BlockSpec(memory_space=pltpu.SMEM)
NT = (((1,), (1,)), ((), ()))


def limit(mib):
    return pltpu.CompilerParams(vmem_limit_bytes=mib << 20)


def silu(v):
    return v / (1.0 + jnp.exp(-v))


def partial_kernel(
    tokens_hbm, gain_hbm, hot_gate_hbm, hot_up_hbm, hot_index_hbm, mask_hbm, cold_gate, cold_up,
    hot_down,
    out, few, live, picks, flag,
    tokens, gain, hot_w, hot_index, mask, normed_v, unit_v, w_v, in_sem, w_sem, row_sem,
    *, slots, block, n_hot, fold,
):
    rows = hot_gate_hbm.shape[0]
    loads = [
        pltpu.make_async_copy(source, target, in_sem.at[i])
        for i, (source, target) in enumerate((
            (mask_hbm, mask), (tokens_hbm, tokens), (gain_hbm, gain),
            (hot_index_hbm, hot_index), (hot_gate_hbm, hot_w.at[pl.ds(0, rows)]),
            (hot_up_hbm, hot_w.at[pl.ds(rows, rows)]),
        ))
    ]
    for load in loads:
        load.start()
    loads[0].wait()
    seqs = tokens.shape[0]
    feats = cold_gate.shape[0]
    blocks = mask.shape[0]
    h = lax.axis_index("hot")
    c = lax.axis_index("cold")
    start = rows * n_hot
    cols = hot_down.shape[1] // n_hot
    chunk = live.shape[0]
    base = start + (rows // chunk * cols if fold else 0)
    mask_f = mask[...].astype(F32)
    alive = jnp.max(mask_f, axis=1, keepdims=True)
    tri = (
        lax.broadcasted_iota(jnp.int32, (blocks, blocks), 1)
        <= lax.broadcasted_iota(jnp.int32, (blocks, blocks), 0)
    ).astype(F32)
    rank = jnp.dot(tri, jnp.broadcast_to(alive, (blocks, block)), preferred_element_type=F32)
    rank = jnp.where(alive > 0.0, rank[:, :1], 0.0)
    number = lax.broadcasted_iota(jnp.int32, (blocks, 1), 0).astype(F32)
    count = jnp.sum(alive).astype(jnp.int32)
    picks[slots] = count
    flag[0] = jnp.where(count <= (few.shape[1] - base) // (2 * block), 1, 0)
    index = []
    for j in range(slots):
        index.append(jnp.sum(jnp.where(rank == float(j + 1), number, 0.0)).astype(jnp.int32))

    def copies(j):
        cols = pl.ds(pl.multiple_of(index[j] * block, block), block)
        return (
            pltpu.make_async_copy(
                cold_gate.at[:, cols], w_v.at[j, :, pl.ds(0, block)], w_sem.at[0, j]
            ),
            pltpu.make_async_copy(
                cold_up.at[:, cols], w_v.at[j, :, pl.ds(block, block)], w_sem.at[1, j]
            ),
        )

    for j in range(slots):
        picks[j] = index[j]

        @pl.when(j < count)
        def _():
            for copy in copies(j):
                copy.start()

    row_copies = []
    if fold:
        for dst in range(n_hot):
            for i in range(rows // chunk):
                row_copies.append(pltpu.make_async_copy(
                    hot_down.at[pl.ds(i * chunk, chunk), pl.ds(dst * cols, cols)],
                    out.at[pl.ds(dst * chunk, chunk), pl.ds(start + i * cols, cols)],
                    row_sem.at[dst, i],
                ))
    for copy in row_copies:
        copy.start()

    loads[1].wait()
    loads[2].wait()
    width = tokens.shape[1]
    squares = jnp.zeros((seqs, block), F32)
    for first in range(0, width, block):
        values = tokens[:, pl.ds(first, block)].astype(F32)
        squares += values * values
    scale = lax.rsqrt(jnp.sum(squares, axis=1, keepdims=True) / width + 1e-05)
    scale = jnp.broadcast_to(scale, (seqs, block))
    for first in range(0, width, block):
        lanes = pl.ds(first, block)
        values = tokens[:, lanes].astype(F32) * scale * gain[:, lanes]
        normed_v[:, lanes] = values.astype(BF16)

    loads[3].wait()
    hidx = hot_index[...] - c * (blocks * block)
    owner = lax.shift_right_arithmetic(hidx, jnp.int32(block.bit_length() - 1))
    inner = jnp.bitwise_and(hidx, jnp.int32(block - 1))
    n = hidx.shape[1]
    by_block = (lax.broadcasted_iota(jnp.int32, (blocks, n), 0) == owner).astype(F32)
    by_unit = (lax.broadcasted_iota(jnp.int32, (block, n), 0) == inner).astype(F32)
    unit_v[...] = 1.0 - lax.dot_general(by_block, by_unit, NT, preferred_element_type=F32)
    mine = (
        lax.broadcasted_iota(jnp.int32, (chunk, seqs), 1)
        == lax.broadcasted_iota(jnp.int32, (chunk, seqs), 0) + h * chunk
    ).astype(F32)
    seq_mask = lax.dot_general(mine, mask_f, NT, preferred_element_type=F32)
    lane = lax.broadcasted_iota(jnp.int32, (1, blocks), 1)
    for j in range(slots):
        seq_live = jnp.sum(
            jnp.where(lane == index[j], seq_mask, 0.0), axis=1, keepdims=True
        ) * jnp.where(j < count, 1.0, 0.0)
        live[:, pl.ds(j * block, block)] = seq_live * unit_v[pl.ds(index[j], 1), :]

    loads[4].wait()
    loads[5].wait()
    both = lax.dot_general(normed_v[...], hot_w[...], NT, preferred_element_type=F32)
    hidden_hot = (silu(both[:, :rows]) * both[:, rows:]).astype(BF16)
    spread = (
        lax.broadcasted_iota(jnp.int32, (rows, rows * n_hot), 1)
        == lax.broadcasted_iota(jnp.int32, (rows, rows * n_hot), 0) + h * rows
    ).astype(BF16)
    out[:, pl.ds(0, rows * n_hot)] = jnp.dot(
        hidden_hot, spread, preferred_element_type=F32
    ).astype(BF16)

    part = normed_v[:, pl.ds(pl.multiple_of(h * feats, feats), feats)]
    for j in range(slots):
        lanes = pl.ds(base + 2 * j * block, 2 * block)

        @pl.when(j < count)
        def _():
            for copy in copies(j):
                copy.wait()
            out[:, lanes] = jnp.dot(part, w_v[j], preferred_element_type=F32).astype(BF16)

        @pl.when(j >= count)
        def _():
            out[:, lanes] = jnp.zeros((seqs, 2 * block), BF16)

    for copy in row_copies:
        copy.wait()

    @pl.when(count <= (few.shape[1] - base) // (2 * block))
    def _():
        few[...] = out[:, pl.ds(0, few.shape[1])]


def hidden_kernel(parts, live, out, *hot_rows, slots, block, n_hot, hot_lanes):
    chunk = live.shape[0]
    base = parts.shape[1] - 2 * slots * block

    def total(start, width):
        lanes = pl.ds(start, width)
        value = parts[pl.ds(0, chunk), lanes].astype(F32)
        for src in range(1, n_hot):
            value = value + parts[pl.ds(src * chunk, chunk), lanes].astype(F32)
        return value

    both = total(base, 2 * slots * block)
    pieces = []
    for j in range(slots):
        gate = both[:, 2 * j * block : (2 * j + 1) * block]
        up = both[:, (2 * j + 1) * block : (2 * j + 2) * block]
        pieces.append((silu(gate) * up * live[:, pl.ds(j * block, block)]).astype(BF16))
    pieces.append(total(0, hot_lanes).astype(BF16))
    hidden = jnp.concatenate(pieces, axis=1)
    for dst in range(n_hot):
        out[pl.ds(dst * chunk, chunk), :] = hidden
    for rows in hot_rows:
        cols = rows.shape[1]
        each = hot_lanes // n_hot // chunk
        for src in range(n_hot):
            for i in range(each):
                rows[pl.ds((src * each + i) * chunk, chunk), :] = parts[
                    pl.ds(src * chunk, chunk), pl.ds(hot_lanes + i * cols, cols)
                ]


def down_kernel(picks, hidden, hot_rows, cold_down, own, *rest, slots, block):
    sends, (total, w, sem) = rest[:-3], rest[-3:]
    count = picks[picks.shape[0] - 1]
    group = 2 if slots % 2 == 0 else 1

    def copy(j):
        rows = pl.ds(pl.multiple_of(picks[j] * block, block), block)
        return pltpu.make_async_copy(cold_down.at[rows], w.at[pl.ds(j * block, block)], sem.at[j])

    for j in range(slots):

        @pl.when(j < count)
        def _():
            copy(j).start()

        @pl.when(j >= count)
        def _():
            w[pl.ds(j * block, block), :] = jnp.zeros((block, w.shape[1]), BF16)

    base = slots * block
    total[...] = jnp.dot(
        hidden[:, pl.ds(base, hot_rows.shape[0])], hot_rows[...], preferred_element_type=F32
    )
    for first in range(0, slots, group):

        @pl.when(first < count)
        def _():
            for j in range(first, first + group):

                @pl.when(j < count)
                def _():
                    copy(j).wait()

            rows = pl.ds(first * block, group * block)
            total[...] += jnp.dot(hidden[:, rows], w[rows, :], preferred_element_type=F32)

    c = lax.axis_index("cold")
    cols = own.shape[1]

    def piece(k):
        if cols % 128 == 0:
            return total[:, pl.ds(pl.multiple_of(k * cols, cols), cols)]
        value = jnp.zeros((total.shape[0], cols), F32)
        for i in range(total.shape[1] // cols):
            value = jnp.where(k == i, total[:, i * cols : (i + 1) * cols], value)
        return value

    own[...] = piece(c)
    for k, send in enumerate(sends):
        send[...] = piece(jnp.bitwise_xor(c, k + 1)).astype(send.dtype)


def in_vmem(value):
    return pltpu.with_memory_space_constraint(value, pltpu.VMEM)


def in_hbm(value):
    return pltpu.with_memory_space_constraint(value, pltpu.HBM)


def on_device(
    tokens, norm_gain, hot_gate, hot_up, hot_down, hot_index,
    cold_gate, cold_up, cold_down, block_mask, *, n_hot, n_cold,
):
    seqs, width = tokens.shape
    feats, units = cold_gate.shape
    blocks = block_mask.shape[1]
    block = units // blocks
    slots = blocks // 2
    rows = hot_gate.shape[0]
    chunk = seqs // n_hot
    hot_lanes = rows * n_hot
    cols = cold_down.shape[1]

    fold = chunk % 8 == 0 and rows % chunk == 0
    row_lanes = rows // chunk * cols if fold else 0
    shared = hot_lanes + row_lanes
    few = max(2, slots // 6 * 2)

    parts, few_parts, live, picks, flag = pl.pallas_call(
        functools.partial(
            partial_kernel, slots=slots, block=block, n_hot=n_hot, fold=fold
        ),
        name="partial",
        compiler_params=limit(20),
        in_specs=[ANY] * 9,
        out_specs=[VMEM, VMEM, VMEM, SMEM, SMEM],
        out_shape=[
            pltpu.VMEM((seqs, shared + 2 * slots * block), BF16),
            pltpu.VMEM((seqs, shared + 2 * few * block), BF16),
            pltpu.VMEM((chunk, slots * block), F32),
            pltpu.SMEM((slots + 1,), jnp.int32),
            pltpu.SMEM((1,), jnp.int32),
        ],
        scratch_shapes=[
            pltpu.VMEM((seqs, width), BF16),
            pltpu.VMEM((1, width), F32),
            pltpu.VMEM((2 * rows, width), BF16),
            pltpu.VMEM((1, hot_index.shape[0]), jnp.int32),
            pltpu.VMEM((blocks, seqs), jnp.int32),
            pltpu.VMEM((seqs, width), BF16),
            pltpu.VMEM((blocks, block), F32),
            pltpu.VMEM((slots, feats, 2 * block), BF16),
            pltpu.SemaphoreType.DMA((6,)),
            pltpu.SemaphoreType.DMA((2, slots)),
            pltpu.SemaphoreType.DMA((n_hot, max(1, rows // chunk))),
        ],
    )(*(in_hbm(value) for value in (
        tokens, norm_gain[None, :], hot_gate, hot_up, hot_index[None, :],
        block_mask.T, cold_gate, cold_up, hot_down,
    )))

    def middle(slots, parts, live, picks, hot_down, cold_down):
        parts = lax.all_to_all(parts, "hot", split_axis=0, concat_axis=0, tiled=True)
        hidden, *moved = pl.pallas_call(
            functools.partial(
                hidden_kernel, slots=slots, block=block, n_hot=n_hot, hot_lanes=hot_lanes
            ),
            name="hidden",
            compiler_params=limit(8),
            in_specs=[VMEM, VMEM],
            out_specs=[VMEM] * (1 + fold),
            out_shape=[
                pltpu.VMEM((seqs, slots * block + hot_lanes), BF16),
                pltpu.VMEM((hot_lanes, cols), BF16),
            ][: 1 + fold],
        )(in_vmem(parts), in_vmem(live))
        if fold:
            hot_rows = moved[0]
        else:
            hot_rows = lax.all_to_all(hot_down, "hot", split_axis=1, concat_axis=0, tiled=True)
        hidden = lax.all_to_all(hidden, "hot", split_axis=0, concat_axis=0, tiled=True)
        piece = (seqs, cols // n_cold)
        return tuple(pl.pallas_call(
            functools.partial(down_kernel, slots=slots, block=block),
            name="down",
            compiler_params=limit(8),
            in_specs=[SMEM, VMEM, VMEM, ANY],
            out_specs=[VMEM] * n_cold,
            out_shape=[pltpu.VMEM(piece, F32)] + [pltpu.VMEM(piece, BF16)] * (n_cold - 1),
            scratch_shapes=[
                pltpu.VMEM((seqs, cols), F32),
                pltpu.VMEM((slots * block, cols), BF16),
                pltpu.SemaphoreType.DMA((slots,)),
            ],
        )(pltpu.with_memory_space_constraint(picks, pltpu.SMEM), in_vmem(hidden), in_vmem(hot_rows), in_hbm(cold_down)))

    own, *sends = lax.cond(
        flag[0] > 0,
        lambda parts, few_parts, *rest: middle(few, few_parts, *rest),
        lambda parts, few_parts, *rest: middle(slots, parts, *rest),
        parts, few_parts, live, picks, hot_down, cold_down,
    )
    for k, send in enumerate(sends):
        got = lax.ppermute(send, "cold", [(i, i ^ (k + 1)) for i in range(n_cold)])
        own = own + got.astype(F32)
    return own.astype(BF16)


def solution(mesh):
    in_specs = (
        P(),
        P(),
        P(("hot", "cold"), None),
        P(("hot", "cold"), None),
        P(("hot", "cold"), None),
        P(),
        P("hot", "cold"),
        P("hot", "cold"),
        P("cold", "hot"),
        P(None, "cold"),
    )

    def body(*args):
        return on_device(*args, n_hot=mesh.shape["hot"], n_cold=mesh.shape["cold"])

    return jax.shard_map(
        body, mesh=mesh, in_specs=in_specs, out_specs=P(None, ("hot", "cold")), check_vma=False
    )
```

```python
import functools

import jax
import jax.numpy as jnp
from jax import lax
from jax.experimental import pallas as pl
from jax.experimental.pallas import tpu as pltpu
from jax.sharding import PartitionSpec as P

F32 = jnp.float32
BF16 = jnp.bfloat16
ANY = pl.BlockSpec(memory_space=pl.ANY)
VMEM = pl.BlockSpec(memory_space=pltpu.VMEM)
SMEM = pl.BlockSpec(memory_space=pltpu.SMEM)
NT = (((1,), (1,)), ((), ()))
EARLY_ALL, EARLY_FEW = True, False


def limit(mib):
    return pltpu.CompilerParams(vmem_limit_bytes=mib << 20)


def silu(v):
    return v / (1.0 + jnp.exp(-v))


def partial_kernel(
    tokens_hbm, gain_hbm, hot_gate_hbm, hot_up_hbm, hot_index_hbm, mask_hbm, cold_gate, cold_up,
    hot_down,
    out, few, late_rows, live, picks, flag,
    tokens, gain, hot_w, hot_index, mask, normed_v, unit_v, w_v, in_sem, w_sem, row_sem,
    *, slots, few_slots, block, n_hot, early,
):
    rows = hot_gate_hbm.shape[0]
    loads = [
        pltpu.make_async_copy(source, target, in_sem.at[i])
        for i, (source, target) in enumerate((
            (mask_hbm, mask), (tokens_hbm, tokens), (gain_hbm, gain),
            (hot_index_hbm, hot_index), (hot_gate_hbm, hot_w.at[pl.ds(0, rows)]),
            (hot_up_hbm, hot_w.at[pl.ds(rows, rows)]),
        ))
    ]
    for load in loads:
        load.start()
    loads[0].wait()
    seqs = tokens.shape[0]
    feats = cold_gate.shape[0]
    blocks = mask.shape[0]
    h = lax.axis_index("hot")
    c = lax.axis_index("cold")
    start = rows * n_hot
    cols = hot_down.shape[1] // n_hot
    chunk = live.shape[0]
    row_lanes = rows // chunk * cols
    base = out.shape[1] - 2 * slots * block
    few_base = few.shape[1] - 2 * few_slots * block
    mask_f = mask[...].astype(F32)
    alive = jnp.max(mask_f, axis=1, keepdims=True)
    tri = (
        lax.broadcasted_iota(jnp.int32, (blocks, blocks), 1)
        <= lax.broadcasted_iota(jnp.int32, (blocks, blocks), 0)
    ).astype(F32)
    rank = jnp.dot(tri, jnp.broadcast_to(alive, (blocks, block)), preferred_element_type=F32)
    rank = jnp.where(alive > 0.0, rank[:, :1], 0.0)
    number = lax.broadcasted_iota(jnp.int32, (blocks, 1), 0).astype(F32)
    count = jnp.sum(alive).astype(jnp.int32)
    picks[slots] = count
    flag[0] = jnp.where(count <= few_slots, 1, 0)
    index = []
    for j in range(slots):
        index.append(jnp.sum(jnp.where(rank == float(j + 1), number, 0.0)).astype(jnp.int32))

    def copies(j):
        cols = pl.ds(pl.multiple_of(index[j] * block, block), block)
        return (
            pltpu.make_async_copy(
                cold_gate.at[:, cols], w_v.at[j, :, pl.ds(0, block)], w_sem.at[0, j]
            ),
            pltpu.make_async_copy(
                cold_up.at[:, cols], w_v.at[j, :, pl.ds(block, block)], w_sem.at[1, j]
            ),
        )

    for j in range(slots):
        picks[j] = index[j]

        @pl.when(j < count)
        def _():
            for copy in copies(j):
                copy.start()

    row_copies = []
    targets = [] if early is None else [(late_rows, 0)] + [(out, start)] * early
    for which, (target, lane0) in enumerate(targets):
        for dst in range(n_hot):
            for i in range(rows // chunk):
                row_copies.append(pltpu.make_async_copy(
                    hot_down.at[pl.ds(i * chunk, chunk), pl.ds(dst * cols, cols)],
                    target.at[pl.ds(dst * chunk, chunk), pl.ds(lane0 + i * cols, cols)],
                    row_sem.at[which, dst, i],
                ))
    for copy in row_copies:
        copy.start()

    loads[1].wait()
    loads[2].wait()
    width = tokens.shape[1]
    squares = jnp.zeros((seqs, block), F32)
    for first in range(0, width, block):
        values = tokens[:, pl.ds(first, block)].astype(F32)
        squares += values * values
    scale = lax.rsqrt(jnp.sum(squares, axis=1, keepdims=True) / width + 1e-05)
    scale = jnp.broadcast_to(scale, (seqs, block))
    for first in range(0, width, block):
        lanes = pl.ds(first, block)
        values = tokens[:, lanes].astype(F32) * scale * gain[:, lanes]
        normed_v[:, lanes] = values.astype(BF16)

    loads[3].wait()
    hidx = hot_index[...] - c * (blocks * block)
    owner = lax.shift_right_arithmetic(hidx, jnp.int32(block.bit_length() - 1))
    inner = jnp.bitwise_and(hidx, jnp.int32(block - 1))
    n = hidx.shape[1]
    by_block = (lax.broadcasted_iota(jnp.int32, (blocks, n), 0) == owner).astype(F32)
    by_unit = (lax.broadcasted_iota(jnp.int32, (block, n), 0) == inner).astype(F32)
    unit_v[...] = 1.0 - lax.dot_general(by_block, by_unit, NT, preferred_element_type=F32)
    mine = (
        lax.broadcasted_iota(jnp.int32, (chunk, seqs), 1)
        == lax.broadcasted_iota(jnp.int32, (chunk, seqs), 0) + h * chunk
    ).astype(F32)
    seq_mask = lax.dot_general(mine, mask_f, NT, preferred_element_type=F32)
    lane = lax.broadcasted_iota(jnp.int32, (1, blocks), 1)
    for j in range(slots):
        seq_live = jnp.sum(
            jnp.where(lane == index[j], seq_mask, 0.0), axis=1, keepdims=True
        ) * jnp.where(j < count, 1.0, 0.0)
        live[:, pl.ds(j * block, block)] = seq_live * unit_v[pl.ds(index[j], 1), :]

    loads[4].wait()
    loads[5].wait()
    both = lax.dot_general(normed_v[...], hot_w[...], NT, preferred_element_type=F32)
    hidden_hot = (silu(both[:, :rows]) * both[:, rows:]).astype(BF16)
    part = chunk if early is not None else rows
    row = lax.broadcasted_iota(jnp.int32, (rows, rows * n_hot), 0)
    place = row // part * (n_hot * part) + h * part + row % part
    spread = (lax.broadcasted_iota(jnp.int32, (rows, rows * n_hot), 1) == place).astype(BF16)
    out[:, pl.ds(0, rows * n_hot)] = jnp.dot(
        hidden_hot, spread, preferred_element_type=F32
    ).astype(BF16)

    part = normed_v[:, pl.ds(pl.multiple_of(h * feats, feats), feats)]
    for j in range(slots):
        lanes = pl.ds(base + 2 * j * block, 2 * block)

        @pl.when(j < count)
        def _():
            for copy in copies(j):
                copy.wait()
            out[:, lanes] = jnp.dot(part, w_v[j], preferred_element_type=F32).astype(BF16)

        @pl.when(j >= count)
        def _():
            out[:, lanes] = jnp.zeros((seqs, 2 * block), BF16)

    for copy in row_copies:
        copy.wait()

    @pl.when(count <= few_slots)
    def _():
        few[:, pl.ds(0, start)] = out[:, pl.ds(0, start)]
        if few_base > start:
            few[:, pl.ds(start, row_lanes)] = late_rows[...]
        lanes = 2 * few_slots * block
        few[:, pl.ds(few_base, lanes)] = out[:, pl.ds(base, lanes)]


def hidden_kernel(parts, live, late_rows, out, *hot_rows, slots, block, n_hot, hot_lanes):
    chunk = live.shape[0]
    base = parts.shape[1] - 2 * slots * block

    def total(start, width):
        lanes = pl.ds(start, width)
        value = parts[pl.ds(0, chunk), lanes].astype(F32)
        for src in range(1, n_hot):
            value = value + parts[pl.ds(src * chunk, chunk), lanes].astype(F32)
        return value

    both = total(base, 2 * slots * block)
    pieces = []
    for j in range(slots):
        gate = both[:, 2 * j * block : (2 * j + 1) * block]
        up = both[:, (2 * j + 1) * block : (2 * j + 2) * block]
        pieces.append((silu(gate) * up * live[:, pl.ds(j * block, block)]).astype(BF16))
    pieces.append(total(0, hot_lanes).astype(BF16))
    hidden = jnp.concatenate(pieces, axis=1)
    width = hidden.shape[1]
    for dst in range(n_hot):
        out[pl.ds(dst * chunk, chunk), pl.ds(0, width)] = hidden
    if out.shape[1] > width:
        out[:, pl.ds(width, late_rows.shape[1])] = late_rows[...]
    for rows in hot_rows:
        seqs, cols = parts.shape[0], rows.shape[1]
        for i in range(rows.shape[0] // seqs):
            rows[pl.ds(i * seqs, seqs), :] = parts[:, pl.ds(hot_lanes + i * cols, cols)]


def down_kernel(picks, hidden, hot_rows, cold_down, own, *rest, slots, block, late):
    sends, (total, w, sem) = rest[:-3], rest[-3:]
    count = picks[picks.shape[0] - 1]
    group = 2 if slots % 2 == 0 else 1

    def copy(j):
        rows = pl.ds(pl.multiple_of(picks[j] * block, block), block)
        return pltpu.make_async_copy(cold_down.at[rows], w.at[pl.ds(j * block, block)], sem.at[j])

    for j in range(slots):

        @pl.when(j < count)
        def _():
            copy(j).start()

        @pl.when(j >= count)
        def _():
            w[pl.ds(j * block, block), :] = jnp.zeros((block, w.shape[1]), BF16)

    base = slots * block
    if late:
        seqs, cols = total.shape
        hot_lanes = hidden.shape[1] - base - late
        total[...] = jnp.zeros(total.shape, F32)
        for i in range(hot_lanes // seqs):
            total[...] += jnp.dot(
                hidden[:, pl.ds(base + i * seqs, seqs)],
                hidden[:, pl.ds(base + hot_lanes + i * cols, cols)],
                preferred_element_type=F32,
            )
    else:
        total[...] = jnp.dot(
            hidden[:, pl.ds(base, hot_rows.shape[0])], hot_rows[...], preferred_element_type=F32
        )
    for first in range(0, slots, group):

        @pl.when(first < count)
        def _():
            for j in range(first, first + group):

                @pl.when(j < count)
                def _():
                    copy(j).wait()

            rows = pl.ds(first * block, group * block)
            total[...] += jnp.dot(hidden[:, rows], w[rows, :], preferred_element_type=F32)

    c = lax.axis_index("cold")
    cols = own.shape[1]

    def piece(k):
        if cols % 128 == 0:
            return total[:, pl.ds(pl.multiple_of(k * cols, cols), cols)]
        value = jnp.zeros((total.shape[0], cols), F32)
        for i in range(total.shape[1] // cols):
            value = jnp.where(k == i, total[:, i * cols : (i + 1) * cols], value)
        return value

    own[...] = piece(c)
    for k, send in enumerate(sends):
        send[...] = piece(jnp.bitwise_xor(c, k + 1)).astype(send.dtype)


def in_vmem(value):
    return pltpu.with_memory_space_constraint(value, pltpu.VMEM)


def in_hbm(value):
    return pltpu.with_memory_space_constraint(value, pltpu.HBM)


def on_device(
    tokens, norm_gain, hot_gate, hot_up, hot_down, hot_index,
    cold_gate, cold_up, cold_down, block_mask, *, n_hot, n_cold,
):
    seqs, width = tokens.shape
    feats, units = cold_gate.shape
    blocks = block_mask.shape[1]
    block = units // blocks
    slots = blocks // 2
    rows = hot_gate.shape[0]
    chunk = seqs // n_hot
    hot_lanes = rows * n_hot
    cols = cold_down.shape[1]

    fold = chunk % 8 == 0 and rows % chunk == 0
    row_lanes = rows // chunk * cols if fold else 0
    few = max(2, slots // 6 * 2)
    early_all, early_few = (EARLY_ALL, EARLY_FEW) if fold else (False, False)

    parts, few_parts, late_rows, live, picks, flag = pl.pallas_call(
        functools.partial(
            partial_kernel, slots=slots, few_slots=few, block=block, n_hot=n_hot,
            early=early_all if fold else None,
        ),
        name="partial",
        compiler_params=limit(20),
        in_specs=[ANY] * 9,
        out_specs=[VMEM] * 4 + [SMEM] * 2,
        out_shape=[
            pltpu.VMEM((seqs, hot_lanes + early_all * row_lanes + 2 * slots * block), BF16),
            pltpu.VMEM((seqs, hot_lanes + early_few * row_lanes + 2 * few * block), BF16),
            pltpu.VMEM((seqs, max(128, row_lanes)), BF16),
            pltpu.VMEM((chunk, slots * block), F32),
            pltpu.SMEM((slots + 1,), jnp.int32),
            pltpu.SMEM((1,), jnp.int32),
        ],
        scratch_shapes=[
            pltpu.VMEM((seqs, width), BF16),
            pltpu.VMEM((1, width), F32),
            pltpu.VMEM((2 * rows, width), BF16),
            pltpu.VMEM((1, hot_index.shape[0]), jnp.int32),
            pltpu.VMEM((blocks, seqs), jnp.int32),
            pltpu.VMEM((seqs, width), BF16),
            pltpu.VMEM((blocks, block), F32),
            pltpu.VMEM((slots, feats, 2 * block), BF16),
            pltpu.SemaphoreType.DMA((6,)),
            pltpu.SemaphoreType.DMA((2, slots)),
            pltpu.SemaphoreType.DMA((2, n_hot, max(1, rows // chunk))),
        ],
    )(*(in_hbm(value) for value in (
        tokens, norm_gain[None, :], hot_gate, hot_up, hot_index[None, :],
        block_mask.T, cold_gate, cold_up, hot_down,
    )))

    def middle(slots, early, parts, late_rows, live, picks, hot_down, cold_down):
        late = 0 if early else row_lanes
        parts = lax.all_to_all(parts, "hot", split_axis=0, concat_axis=0, tiled=True)
        hidden, *moved = pl.pallas_call(
            functools.partial(
                hidden_kernel, slots=slots, block=block, n_hot=n_hot, hot_lanes=hot_lanes
            ),
            name="hidden",
            compiler_params=limit(8),
            in_specs=[VMEM] * 3,
            out_specs=[VMEM] * (1 + early),
            out_shape=[
                pltpu.VMEM((seqs, slots * block + hot_lanes + late), BF16),
                pltpu.VMEM((hot_lanes, cols), BF16),
            ][: 1 + early],
        )(in_vmem(parts), in_vmem(live), in_vmem(late_rows))
        if early:
            hot_rows = moved[0]
        elif late:
            hot_rows = late_rows
        else:
            hot_rows = lax.all_to_all(hot_down, "hot", split_axis=1, concat_axis=0, tiled=True)
        hidden = lax.all_to_all(hidden, "hot", split_axis=0, concat_axis=0, tiled=True)
        piece = (seqs, cols // n_cold)
        return tuple(pl.pallas_call(
            functools.partial(down_kernel, slots=slots, block=block, late=late),
            name="down",
            compiler_params=limit(8),
            in_specs=[SMEM, VMEM, VMEM, ANY],
            out_specs=[VMEM] * n_cold,
            out_shape=[pltpu.VMEM(piece, F32)] + [pltpu.VMEM(piece, BF16)] * (n_cold - 1),
            scratch_shapes=[
                pltpu.VMEM((seqs, cols), F32),
                pltpu.VMEM((slots * block, cols), BF16),
                pltpu.SemaphoreType.DMA((slots,)),
            ],
        )(pltpu.with_memory_space_constraint(picks, pltpu.SMEM), in_vmem(hidden), in_vmem(hot_rows), in_hbm(cold_down)))

    own, *sends = lax.cond(
        flag[0] > 0,
        lambda parts, few_parts, *rest: middle(few, early_few, few_parts, *rest),
        lambda parts, few_parts, *rest: middle(slots, early_all, parts, *rest),
        parts, few_parts, late_rows, live, picks, hot_down, cold_down,
    )
    for k, send in enumerate(sends):
        got = lax.ppermute(send, "cold", [(i, i ^ (k + 1)) for i in range(n_cold)])
        own = own + got.astype(F32)
    return own.astype(BF16)


def solution(mesh):
    in_specs = (
        P(),
        P(),
        P(("hot", "cold"), None),
        P(("hot", "cold"), None),
        P(("hot", "cold"), None),
        P(),
        P("hot", "cold"),
        P("hot", "cold"),
        P("cold", "hot"),
        P(None, "cold"),
    )

    def body(*args):
        return on_device(*args, n_hot=mesh.shape["hot"], n_cold=mesh.shape["cold"])

    return jax.shard_map(
        body, mesh=mesh, in_specs=in_specs, out_specs=P(None, ("hot", "cold")), check_vma=False
    )
```

```python
import functools

import jax
import jax.numpy as jnp
from jax import lax
from jax.experimental import pallas as pl
from jax.experimental.pallas import tpu as pltpu
from jax.sharding import PartitionSpec as P

F32 = jnp.float32
BF16 = jnp.bfloat16
ANY = pl.BlockSpec(memory_space=pl.ANY)
VMEM = pl.BlockSpec(memory_space=pltpu.VMEM)
SMEM = pl.BlockSpec(memory_space=pltpu.SMEM)
NT = (((1,), (1,)), ((), ()))


def limit(mib):
    return pltpu.CompilerParams(vmem_limit_bytes=mib << 20)


def silu(v):
    return v / (1.0 + jnp.exp(-v))


def partial_kernel(
    tokens_hbm, gain_hbm, hot_gate_hbm, hot_up_hbm, hot_index_hbm, mask_hbm, cold_gate, cold_up,
    hot_down,
    wide, out, few_wide, few, row_out, live, picks, branch,
    tokens, gain, hot_w, hot_index, mask, normed_v, unit_v, w_v, in_sem, w_sem, row_sem,
    *, slots, few_slots, block, n_hot, fold,
):
    rows = hot_gate_hbm.shape[0]
    loads = [
        pltpu.make_async_copy(source, target, in_sem.at[i])
        for i, (source, target) in enumerate((
            (mask_hbm, mask), (tokens_hbm, tokens), (gain_hbm, gain),
            (hot_index_hbm, hot_index), (hot_gate_hbm, hot_w.at[pl.ds(0, rows)]),
            (hot_up_hbm, hot_w.at[pl.ds(rows, rows)]),
        ))
    ]
    for load in loads:
        load.start()
    loads[0].wait()
    seqs = tokens.shape[0]
    feats = cold_gate.shape[0]
    blocks = mask.shape[0]
    h = lax.axis_index("hot")
    c = lax.axis_index("cold")
    start = rows * n_hot
    cols = hot_down.shape[1] // n_hot
    chunk = live.shape[0]
    base = start
    mask_f = mask[...].astype(F32)
    alive = jnp.max(mask_f, axis=1, keepdims=True)
    tri = (
        lax.broadcasted_iota(jnp.int32, (blocks, blocks), 1)
        <= lax.broadcasted_iota(jnp.int32, (blocks, blocks), 0)
    ).astype(F32)
    rank = jnp.dot(tri, jnp.broadcast_to(alive, (blocks, block)), preferred_element_type=F32)
    rank = jnp.where(alive > 0.0, rank[:, :1], 0.0)
    number = lax.broadcasted_iota(jnp.int32, (blocks, 1), 0).astype(F32)
    count = jnp.sum(alive).astype(jnp.int32)
    picks[slots] = count
    branch[0] = jnp.where(count <= few_slots, 0, 1) + 2 * (c % 2)
    index = []
    for j in range(slots):
        index.append(jnp.sum(jnp.where(rank == float(j + 1), number, 0.0)).astype(jnp.int32))

    def copies(j):
        cols = pl.ds(pl.multiple_of(index[j] * block, block), block)
        return (
            pltpu.make_async_copy(
                cold_gate.at[:, cols], w_v.at[j, :, pl.ds(0, block)], w_sem.at[0, j]
            ),
            pltpu.make_async_copy(
                cold_up.at[:, cols], w_v.at[j, :, pl.ds(block, block)], w_sem.at[1, j]
            ),
        )

    for j in range(slots):
        picks[j] = index[j]

        @pl.when(j < count)
        def _():
            for copy in copies(j):
                copy.start()

    row_copies = []
    if fold:
        for dst in range(n_hot):
            for i in range(rows // chunk):
                row_copies.append(pltpu.make_async_copy(
                    hot_down.at[pl.ds(i * chunk, chunk), pl.ds(dst * cols, cols)],
                    row_out.at[pl.ds(dst * chunk, chunk), pl.ds(i * cols, cols)],
                    row_sem.at[dst, i],
                ))
    for copy in row_copies:
        copy.start()

    loads[1].wait()
    loads[2].wait()
    width = tokens.shape[1]
    squares = jnp.zeros((seqs, block), F32)
    for first in range(0, width, block):
        values = tokens[:, pl.ds(first, block)].astype(F32)
        squares += values * values
    scale = lax.rsqrt(jnp.sum(squares, axis=1, keepdims=True) / width + 1e-05)
    scale = jnp.broadcast_to(scale, (seqs, block))
    for first in range(0, width, block):
        lanes = pl.ds(first, block)
        values = tokens[:, lanes].astype(F32) * scale * gain[:, lanes]
        normed_v[:, lanes] = values.astype(BF16)

    loads[3].wait()
    hidx = hot_index[...] - c * (blocks * block)
    owner = lax.shift_right_arithmetic(hidx, jnp.int32(block.bit_length() - 1))
    inner = jnp.bitwise_and(hidx, jnp.int32(block - 1))
    n = hidx.shape[1]
    by_block = (lax.broadcasted_iota(jnp.int32, (blocks, n), 0) == owner).astype(F32)
    by_unit = (lax.broadcasted_iota(jnp.int32, (block, n), 0) == inner).astype(F32)
    unit_v[...] = 1.0 - lax.dot_general(by_block, by_unit, NT, preferred_element_type=F32)
    mine = (
        lax.broadcasted_iota(jnp.int32, (chunk, seqs), 1)
        == lax.broadcasted_iota(jnp.int32, (chunk, seqs), 0) + h * chunk
    ).astype(F32)
    seq_mask = lax.dot_general(mine, mask_f, NT, preferred_element_type=F32)
    lane = lax.broadcasted_iota(jnp.int32, (1, blocks), 1)
    for j in range(slots):
        seq_live = jnp.sum(
            jnp.where(lane == index[j], seq_mask, 0.0), axis=1, keepdims=True
        ) * jnp.where(j < count, 1.0, 0.0)
        live[:, pl.ds(j * block, block)] = seq_live * unit_v[pl.ds(index[j], 1), :]

    loads[4].wait()
    loads[5].wait()
    both = lax.dot_general(normed_v[...], hot_w[...], NT, preferred_element_type=F32)
    hidden_hot = (silu(both[:, :rows]) * both[:, rows:]).astype(BF16)
    part = chunk if fold else rows
    row = lax.broadcasted_iota(jnp.int32, (rows, rows * n_hot), 0)
    place = row // part * (n_hot * part) + h * part + row % part
    spread = (lax.broadcasted_iota(jnp.int32, (rows, rows * n_hot), 1) == place).astype(BF16)
    out[:, pl.ds(0, rows * n_hot)] = jnp.dot(
        hidden_hot, spread, preferred_element_type=F32
    ).astype(BF16)

    part = normed_v[:, pl.ds(pl.multiple_of(h * feats, feats), feats)]
    for j in range(slots):
        lanes = pl.ds(base + 2 * j * block, 2 * block)

        @pl.when(j < count)
        def _():
            for copy in copies(j):
                copy.wait()
            out[:, lanes] = jnp.dot(part, w_v[j], preferred_element_type=F32).astype(BF16)

        @pl.when(j >= count)
        def _():
            out[:, lanes] = jnp.zeros((seqs, 2 * block), BF16)

    for copy in row_copies:
        copy.wait()

    def fill(target, lanes):
        target[:, pl.ds(0, start)] = out[:, pl.ds(0, start)]
        shift = target.shape[1] - start - lanes
        if shift:
            target[:, pl.ds(start, shift)] = row_out[...]
        target[:, pl.ds(start + shift, lanes)] = out[:, pl.ds(start, lanes)]

    @pl.when(branch[0] == 0)
    def _():
        fill(few, 2 * few_slots * block)

    @pl.when(branch[0] == 2)
    def _():
        fill(few_wide, 2 * few_slots * block)

    @pl.when(branch[0] == 3)
    def _():
        fill(wide, 2 * slots * block)


def hidden_kernel(parts, live, late_rows, out, *hot_rows, slots, block, n_hot, hot_lanes):
    chunk = live.shape[0]
    base = parts.shape[1] - 2 * slots * block

    def total(start, width):
        lanes = pl.ds(start, width)
        value = parts[pl.ds(0, chunk), lanes].astype(F32)
        for src in range(1, n_hot):
            value = value + parts[pl.ds(src * chunk, chunk), lanes].astype(F32)
        return value

    both = total(base, 2 * slots * block)
    pieces = []
    for j in range(slots):
        gate = both[:, 2 * j * block : (2 * j + 1) * block]
        up = both[:, (2 * j + 1) * block : (2 * j + 2) * block]
        pieces.append((silu(gate) * up * live[:, pl.ds(j * block, block)]).astype(BF16))
    pieces.append(total(0, hot_lanes).astype(BF16))
    hidden = jnp.concatenate(pieces, axis=1)
    width = hidden.shape[1]
    for dst in range(n_hot):
        out[pl.ds(dst * chunk, chunk), pl.ds(0, width)] = hidden
    if out.shape[1] > width:
        out[:, pl.ds(width, late_rows.shape[1])] = late_rows[...]
    for rows in hot_rows:
        seqs, cols = parts.shape[0], rows.shape[1]
        for i in range(rows.shape[0] // seqs):
            rows[pl.ds(i * seqs, seqs), :] = parts[:, pl.ds(hot_lanes + i * cols, cols)]


def down_kernel(picks, hidden, hot_rows, cold_down, own, *rest, slots, block, late):
    sends, (total, w, sem) = rest[:-3], rest[-3:]
    count = picks[picks.shape[0] - 1]
    group = 2 if slots % 2 == 0 else 1

    def copy(j):
        rows = pl.ds(pl.multiple_of(picks[j] * block, block), block)
        return pltpu.make_async_copy(cold_down.at[rows], w.at[pl.ds(j * block, block)], sem.at[j])

    for j in range(slots):

        @pl.when(j < count)
        def _():
            copy(j).start()

        @pl.when(j >= count)
        def _():
            w[pl.ds(j * block, block), :] = jnp.zeros((block, w.shape[1]), BF16)

    base = slots * block
    if late:
        seqs, cols = total.shape
        hot_lanes = hidden.shape[1] - base - late
        total[...] = jnp.zeros(total.shape, F32)
        for i in range(hot_lanes // seqs):
            total[...] += jnp.dot(
                hidden[:, pl.ds(base + i * seqs, seqs)],
                hidden[:, pl.ds(base + hot_lanes + i * cols, cols)],
                preferred_element_type=F32,
            )
    else:
        total[...] = jnp.dot(
            hidden[:, pl.ds(base, hot_rows.shape[0])], hot_rows[...], preferred_element_type=F32
        )
    for first in range(0, slots, group):

        @pl.when(first < count)
        def _():
            for j in range(first, first + group):

                @pl.when(j < count)
                def _():
                    copy(j).wait()

            rows = pl.ds(first * block, group * block)
            total[...] += jnp.dot(hidden[:, rows], w[rows, :], preferred_element_type=F32)

    c = lax.axis_index("cold")
    cols = own.shape[1]

    def piece(k):
        if cols % 128 == 0:
            return total[:, pl.ds(pl.multiple_of(k * cols, cols), cols)]
        value = jnp.zeros((total.shape[0], cols), F32)
        for i in range(total.shape[1] // cols):
            value = jnp.where(k == i, total[:, i * cols : (i + 1) * cols], value)
        return value

    own[...] = piece(c)
    for k, send in enumerate(sends):
        send[...] = piece(jnp.bitwise_xor(c, k + 1)).astype(send.dtype)


def in_vmem(value):
    return pltpu.with_memory_space_constraint(value, pltpu.VMEM)


def in_hbm(value):
    return pltpu.with_memory_space_constraint(value, pltpu.HBM)


def on_device(
    tokens, norm_gain, hot_gate, hot_up, hot_down, hot_index,
    cold_gate, cold_up, cold_down, block_mask, *, n_hot, n_cold,
):
    seqs, width = tokens.shape
    feats, units = cold_gate.shape
    blocks = block_mask.shape[1]
    block = units // blocks
    slots = blocks // 2
    rows = hot_gate.shape[0]
    chunk = seqs // n_hot
    hot_lanes = rows * n_hot
    cols = cold_down.shape[1]

    fold = chunk % 8 == 0 and rows % chunk == 0
    row_lanes = rows // chunk * cols if fold else 0
    few = max(2, slots // 6 * 2)

    *sent, late_rows, live, picks, branch = pl.pallas_call(
        functools.partial(
            partial_kernel, slots=slots, few_slots=few, block=block, n_hot=n_hot,
            fold=fold,
        ),
        name="partial",
        compiler_params=limit(20),
        in_specs=[ANY] * 9,
        out_specs=[VMEM] * 6 + [SMEM] * 2,
        out_shape=[
            pltpu.VMEM((seqs, hot_lanes + row_lanes + 2 * slots * block), BF16),
            pltpu.VMEM((seqs, hot_lanes + 2 * slots * block), BF16),
            pltpu.VMEM((seqs, hot_lanes + row_lanes + 2 * few * block), BF16),
            pltpu.VMEM((seqs, hot_lanes + 2 * few * block), BF16),
            pltpu.VMEM((seqs, max(128, row_lanes)), BF16),
            pltpu.VMEM((chunk, slots * block), F32),
            pltpu.SMEM((slots + 1,), jnp.int32),
            pltpu.SMEM((1,), jnp.int32),
        ],
        scratch_shapes=[
            pltpu.VMEM((seqs, width), BF16),
            pltpu.VMEM((1, width), F32),
            pltpu.VMEM((2 * rows, width), BF16),
            pltpu.VMEM((1, hot_index.shape[0]), jnp.int32),
            pltpu.VMEM((blocks, seqs), jnp.int32),
            pltpu.VMEM((seqs, width), BF16),
            pltpu.VMEM((blocks, block), F32),
            pltpu.VMEM((slots, feats, 2 * block), BF16),
            pltpu.SemaphoreType.DMA((6,)),
            pltpu.SemaphoreType.DMA((2, slots)),
            pltpu.SemaphoreType.DMA((n_hot, max(1, rows // chunk))),
        ],
    )(*(in_hbm(value) for value in (
        tokens, norm_gain[None, :], hot_gate, hot_up, hot_index[None, :],
        block_mask.T, cold_gate, cold_up, hot_down,
    )))

    def middle(slots, early, parts, late_rows, live, picks, hot_down, cold_down):
        late = 0 if early else row_lanes
        parts = lax.all_to_all(parts, "hot", split_axis=0, concat_axis=0, tiled=True)
        hidden, *moved = pl.pallas_call(
            functools.partial(
                hidden_kernel, slots=slots, block=block, n_hot=n_hot, hot_lanes=hot_lanes
            ),
            name="hidden",
            compiler_params=limit(8),
            in_specs=[VMEM] * 3,
            out_specs=[VMEM] * (1 + early),
            out_shape=[
                pltpu.VMEM((seqs, slots * block + hot_lanes + late), BF16),
                pltpu.VMEM((hot_lanes, cols), BF16),
            ][: 1 + early],
        )(in_vmem(parts), in_vmem(live), in_vmem(late_rows))
        if early:
            hot_rows = moved[0]
        elif late:
            hot_rows = late_rows
        else:
            hot_rows = lax.all_to_all(hot_down, "hot", split_axis=1, concat_axis=0, tiled=True)
        hidden = lax.all_to_all(hidden, "hot", split_axis=0, concat_axis=0, tiled=True)
        piece = (seqs, cols // n_cold)
        return tuple(pl.pallas_call(
            functools.partial(down_kernel, slots=slots, block=block, late=late),
            name="down",
            compiler_params=limit(8),
            in_specs=[SMEM, VMEM, VMEM, ANY],
            out_specs=[VMEM] * n_cold,
            out_shape=[pltpu.VMEM(piece, F32)] + [pltpu.VMEM(piece, BF16)] * (n_cold - 1),
            scratch_shapes=[
                pltpu.VMEM((seqs, cols), F32),
                pltpu.VMEM((slots * block, cols), BF16),
                pltpu.SemaphoreType.DMA((slots,)),
            ],
        )(pltpu.with_memory_space_constraint(picks, pltpu.SMEM), in_vmem(hidden), in_vmem(hot_rows), in_hbm(cold_down)))

    wide, narrow, few_wide, few_narrow = sent
    own, *sends = lax.switch(
        branch[0],
        [
            lambda wide, narrow, few_wide, few_narrow, *rest: middle(few, False, few_narrow, *rest),
            lambda wide, narrow, few_wide, few_narrow, *rest: middle(slots, False, narrow, *rest),
            lambda wide, narrow, few_wide, few_narrow, *rest: middle(few, fold, few_wide, *rest),
            lambda wide, narrow, few_wide, few_narrow, *rest: middle(slots, fold, wide, *rest),
        ],
        wide, narrow, few_wide, few_narrow, late_rows, live, picks, hot_down, cold_down,
    )
    for k in [*range(1, n_cold - 1), 0]:
        send = sends[k]
        got = lax.ppermute(send, "cold", [(i, i ^ (k + 1)) for i in range(n_cold)])
        own = own + got.astype(F32)
    return own.astype(BF16)


def solution(mesh):
    in_specs = (
        P(),
        P(),
        P(("hot", "cold"), None),
        P(("hot", "cold"), None),
        P(("hot", "cold"), None),
        P(),
        P("hot", "cold"),
        P("hot", "cold"),
        P("cold", "hot"),
        P(None, "cold"),
    )

    def body(*args):
        return on_device(*args, n_hot=mesh.shape["hot"], n_cold=mesh.shape["cold"])

    return jax.shard_map(
        body, mesh=mesh, in_specs=in_specs, out_specs=P(None, ("hot", "cold")), check_vma=False
    )
```
